32 devices in a mesh: dp: 2 (over x), fsdp: 4 (over z), sp: 4 (over y, core).
Axes of the slice: x: 2, y: 2, z: 4, core: 2. Of those that a mesh axis runs over, the one named last changes fastest.
Arguments:
- x_in: bfloat16 [96, 256, 2560], P(('dp', 'fsdp'), 'sp'), parts along dimension 0
- norm_attn: bfloat16 [2560], P('fsdp')
- w_query: bfloat16 [2560, 2560], P('fsdp')
- w_key: bfloat16 [2560, 2560], P('fsdp')
- w_value: bfloat16 [2560, 2560], P('fsdp')
- w_out: bfloat16 [2560, 2560], P('fsdp')
- norm_mlp: bfloat16 [2560], P('fsdp')
- w_gate: bfloat16 [2560, 6912], P('fsdp')
- w_up: bfloat16 [2560, 6912], P('fsdp')
- w_down: bfloat16 [6912, 2560], P('fsdp')
Outputs:
- output: bfloat16 [96, 256, 2560], P(('dp', 'fsdp'), 'sp'), parts along dimension 0
There are 2 independent parts. The reference program is written for one: setup_inputs(seed, part) draws one part's arguments, and reference() takes and returns one part's arrays. A program takes and returns all parts, laid end to end along the dimension named above; an argument that names none is the same for every part.
All inputs are finite; a program needn't handle non-finite values.
Results may differ from the reference program's by a relative error of at most 0.0114395.
Values are sent between devices in bfloat16 or wider.
A program may use at most 1 GiB of HBM per device.

```python
import math
import jax
import jax.numpy as jnp
from jax import lax

MODEL_DIM = 2560
NUM_HEADS = 20
FFN_DIM = 6912
NUM_ROWS = 48
SEQ_SHARDS = 4
SHARD_LEN = 64
QUERY_BLOCK = 32

HEAD_DIM = MODEL_DIM // NUM_HEADS
SEQ_LEN = SEQ_SHARDS * SHARD_LEN
ANCHOR_GAP = 2 * SEQ_SHARDS
NORM_EPS = 1e-5
ROPE_THETA = 5e7
MASK_VALUE = -1e30


def dealt_order(natural):
    lead_rows = natural.shape[0]
    tail_shape = natural.shape[2:]
    token_grid = natural.reshape((lead_rows, SHARD_LEN, SEQ_SHARDS) + tail_shape)
    return jnp.swapaxes(token_grid, 1, 2).reshape((lead_rows, SEQ_LEN) + tail_shape)


def draw_tokens(rng_key):
    key_anchor, key_noise = jax.random.split(rng_key)
    anchors = jax.random.normal(key_anchor, (NUM_ROWS, SEQ_LEN // ANCHOR_GAP + 1, MODEL_DIM), jnp.float32)
    ramp_wts = (jnp.arange(ANCHOR_GAP, dtype=jnp.float32) / ANCHOR_GAP)[None, None, :, None]
    smooth = (1.0 - ramp_wts) * anchors[:, :-1, None, :] + ramp_wts * anchors[:, 1:, None, :]
    smooth = smooth.reshape(NUM_ROWS, SEQ_LEN, MODEL_DIM)
    noise_part = jax.random.normal(key_noise, (NUM_ROWS, SEQ_LEN, MODEL_DIM), jnp.float32)
    return dealt_order(smooth + 0.3 * noise_part).astype(jnp.bfloat16)


def draw_matrix(rng_key, fan_in, fan_out):
    return jax.random.normal(rng_key, (fan_in, fan_out), jnp.float32) * fan_in ** -0.5


def draw_gain(rng_key):
    return jax.random.uniform(rng_key, (MODEL_DIM,), jnp.float32, 0.5, 1.5).astype(jnp.bfloat16)


def setup_inputs(seed: int = 0, part: int = 0) -> dict:
    root_key = jax.random.key(seed)
    shared_keys = jax.random.split(jax.random.fold_in(root_key, 100003), 9)
    query_w = draw_matrix(shared_keys[1], MODEL_DIM, MODEL_DIM)
    key_w = 0.8 * query_w + 0.6 * draw_matrix(shared_keys[2], MODEL_DIM, MODEL_DIM)
    return {
        'x_in': draw_tokens(jax.random.fold_in(root_key, part)),
        'norm_attn': draw_gain(shared_keys[0]),
        'w_query': query_w.astype(jnp.bfloat16),
        'w_key': key_w.astype(jnp.bfloat16),
        'w_value': draw_matrix(shared_keys[3], MODEL_DIM, MODEL_DIM).astype(jnp.bfloat16),
        'w_out': draw_matrix(shared_keys[4], MODEL_DIM, MODEL_DIM).astype(jnp.bfloat16),
        'norm_mlp': draw_gain(shared_keys[5]),
        'w_gate': draw_matrix(shared_keys[6], MODEL_DIM, FFN_DIM).astype(jnp.bfloat16),
        'w_up': draw_matrix(shared_keys[7], MODEL_DIM, FFN_DIM).astype(jnp.bfloat16),
        'w_down': draw_matrix(shared_keys[8], FFN_DIM, MODEL_DIM).astype(jnp.bfloat16),
    }


def rms_norm(hidden, gain):
    hid_f32 = hidden.astype(jnp.float32)
    inv_rms = lax.rsqrt(jnp.mean(hid_f32 * hid_f32, axis=-1, keepdims=True) + NORM_EPS)
    return (hid_f32 * inv_rms * gain.astype(jnp.float32)).astype(jnp.bfloat16)


def apply_rope(proj, angles):
    half_dim = proj.shape[-1] // 2
    lower_half = proj[..., :half_dim]
    upper_half = proj[..., half_dim:]
    cos_tab = jnp.cos(angles)[..., None, :]
    sin_tab = jnp.sin(angles)[..., None, :]
    return jnp.concatenate([lower_half * cos_tab - upper_half * sin_tab, upper_half * cos_tab + lower_half * sin_tab], axis=-1)


def reference(x_in, norm_attn, w_query, w_key, w_value, w_out, norm_mlp, w_gate, w_up, w_down):
    score_scale = HEAD_DIM ** -0.5
    num_blocks = SEQ_LEN // QUERY_BLOCK
    head_shape = (SEQ_LEN, NUM_HEADS, HEAD_DIM)
    seq_idx = jnp.arange(SEQ_LEN, dtype=jnp.int32)
    row_pos = (seq_idx % SHARD_LEN) * SEQ_SHARDS + seq_idx // SHARD_LEN
    inv_freq = jnp.exp(jnp.arange(HEAD_DIM // 2, dtype=jnp.float32) * (-2.0 * math.log(ROPE_THETA) / HEAD_DIM))
    angles = row_pos.astype(jnp.float32)[:, None] * inv_freq[None, :]
    query_pos = row_pos.reshape(num_blocks, QUERY_BLOCK)

    def row_layer(hidden):
        normed = rms_norm(hidden, norm_attn)
        query_rot = apply_rope(jnp.dot(normed, w_query, preferred_element_type=jnp.float32).reshape(head_shape), angles).astype(jnp.bfloat16)
        key_f32 = apply_rope(jnp.dot(normed, w_key, preferred_element_type=jnp.float32).reshape(head_shape), angles).astype(jnp.bfloat16).astype(jnp.float32)
        value_f32 = jnp.dot(normed, w_value, preferred_element_type=jnp.float32).astype(jnp.bfloat16).astype(jnp.float32).reshape(head_shape)

        def block_layer(block_args):
            hid_blk, query_blk, qpos_blk = block_args
            scores = jnp.einsum('qhd,khd->hqk', query_blk.astype(jnp.float32), key_f32) * score_scale
            allowed = row_pos[None, None, :] <= qpos_blk[None, :, None]
            attn_prob = jax.nn.softmax(jnp.where(allowed, scores, MASK_VALUE), axis=-1)
            attn_mix = jnp.einsum('hqk,khd->qhd', attn_prob, value_f32).astype(jnp.bfloat16).reshape(QUERY_BLOCK, MODEL_DIM)
            resid_blk = (hid_blk.astype(jnp.float32) + jnp.dot(attn_mix, w_out, preferred_element_type=jnp.float32)).astype(jnp.bfloat16)
            normed_mlp = rms_norm(resid_blk, norm_mlp)
            gate_act = jax.nn.silu(jnp.dot(normed_mlp, w_gate, preferred_element_type=jnp.float32))
            up_proj = jnp.dot(normed_mlp, w_up, preferred_element_type=jnp.float32)
            hidden_mlp = (gate_act * up_proj).astype(jnp.bfloat16)
            return (resid_blk.astype(jnp.float32) + jnp.dot(hidden_mlp, w_down, preferred_element_type=jnp.float32)).astype(jnp.bfloat16)

        blocks = (hidden.reshape(num_blocks, QUERY_BLOCK, MODEL_DIM), query_rot.reshape(num_blocks, QUERY_BLOCK, NUM_HEADS, HEAD_DIM), query_pos)
        return lax.map(block_layer, blocks).reshape(SEQ_LEN, MODEL_DIM)

    return lax.map(row_layer, x_in)
```

```python
import math
import functools
import jax
import jax.numpy as jnp
from jax import lax
from jax.experimental import pallas as pl
from jax.experimental.pallas import tpu as pltpu
from jax.sharding import PartitionSpec as P

HEAD_DIM = 128
NORM_EPS = 1e-5
ROPE_THETA = 5e7
MASK_VALUE = -1e30
MESH = pl.DeviceIdType.MESH
NZ = 4
SP = 4
PER = 3
BLK = 64
SEQ = SP * BLK
TOK = PER * SEQ
DIM = 2560
FFN = 6912
HALF = DIM // 2
TILE = 256
N_KINDS = 14
SLOTS = 8
AHEAD = 2
LAG = 3
W_Q, W_K, W_V, W_O, W_G, W_U, W_D = range(7)


def split_rows(block):
    over_z = block // 10 // 8 * 8
    over_x = (block - over_z) * 11 // 20 // 8 * 8
    return over_z, over_x


def remote(src, dst, send_sem, recv_sem, dev):
    return pltpu.make_async_remote_copy(
        src_ref=src, dst_ref=dst, send_sem=send_sem, recv_sem=recv_sem, device_id=dev, device_id_type=MESH)


class Mover:
    def __init__(self, shards, gathered, rounds, send_sem, recv_sem):
        self.shards, self.gathered, self.rounds = shards, gathered, rounds
        self.send_sem, self.recv_sem = send_sem, recv_sem
        dx, fz, s = lax.axis_index('dp'), lax.axis_index('fsdp'), lax.axis_index('sp')
        self.dx, self.fz, self.s = dx, fz, s
        self.y, self.c = lax.div(s, 2), lax.rem(s, 2)
        self.core_dev = (dx, fz, self.y * 2 + (1 - self.c))
        self.x_dev = (1 - dx, fz, s)
        self.y_dev = (dx, fz, (1 - self.y) * 2 + self.c)

    def block(self, dx, y, c):
        return (dx * 2 + y) * 2 + c

    def copies(self, r, stage):
        w, lo, width = self.rounds[r]
        sh, g = self.shards[w], self.gathered[w]
        rb = sh.shape[0] // 8
        cols = pl.ds(lo, width)
        az, ax = split_rows(rb)
        dx, y, c = self.dx, self.y, self.c
        mine = self.block(dx, y, c)
        diag = self.block(1 - dx, 1 - y, c)
        xblk, yblk = self.block(1 - dx, y, c), self.block(dx, 1 - y, c)
        slot = r % SLOTS
        out = []

        def rows(blk, a, b):
            return pl.ds(pl.multiple_of(blk * rb + a, 8), b - a)

        def add(kind, src, dst, dev):
            out.append(remote(src, dst, self.send_sem.at[slot, kind], self.recv_sem.at[slot, kind], dev))

        def same(kind, blk, a, b, dev):
            ref = g.at[1:NZ, rows(blk, a, b), cols]
            add(kind, ref, ref, dev)

        if stage == 'z':
            for k in range(1, NZ):
                dev = (dx, lax.rem(self.fz + k, NZ), self.s)
                add(k - 1, sh.at[rows(mine, 0, rb), cols], g.at[NZ - k, rows(mine, 0, rb), cols], dev)
                add(k + 2, sh.at[rows(diag, 0, az), cols], g.at[NZ - k, rows(diag, 0, az), cols], dev)
        if stage == 'p1':
            same(6, mine, 0, rb, self.x_dev)
            same(7, mine, 0, rb, self.y_dev)
        if stage == 'p1c':
            same(8, mine, 0, rb, self.core_dev)
        if stage == 'p2':
            same(9, yblk, az, az + ax, self.x_dev)
            same(10, xblk, az + ax, rb, self.y_dev)
        if stage == 'p2c':
            same(11, xblk, 0, rb, self.core_dev)
            same(12, yblk, 0, rb, self.core_dev)
        if stage == 'p3':
            same(13, diag, 0, rb, self.core_dev)
        return out

    def start(self, r, *stages):
        if 0 <= r < len(self.rounds):
            for stage in stages:
                for cp in self.copies(r, stage):
                    cp.start()

    def wait_recv(self, r, *stages):
        if 0 <= r < len(self.rounds):
            for stage in stages:
                for cp in self.copies(r, stage):
                    cp.wait_recv()

    def wait_send(self, r):
        if 0 <= r < len(self.rounds):
            for stage in ('z', 'p1', 'p1c', 'p2', 'p2c', 'p3'):
                for cp in self.copies(r, stage):
                    cp.wait_send()

    def step(self, i):
        if i == 0:
            for r in range(AHEAD):
                self.start(r, 'z')
        self.wait_send(i + AHEAD - SLOTS)
        self.start(i + AHEAD, 'z')
        self.wait_recv(i, 'z')
        self.start(i, 'p1', 'p1c')
        self.wait_recv(i - 1, 'p1')
        self.start(i - 1, 'p2', 'p2c')
        self.wait_recv(i - 2, 'p2')
        self.start(i - 2, 'p3')
        self.wait_recv(i - 3, 'p1c', 'p2c', 'p3')

    def ticks(self):
        return len(self.rounds) + LAG

    def finish(self):
        n = len(self.rounds)
        done = n + LAG + AHEAD - SLOTS
        for r in range(max(done, 0), n):
            self.wait_send(r)


def plan():
    rounds = []
    for half in range(2):
        rounds += [(w, half * HALF, HALF) for w in (W_Q, W_K, W_V)]
    rounds += [(W_O, 0, HALF), (W_O, HALF, HALF)]
    for c in range(9):
        rounds += [(W_G, c * 768, 768), (W_U, c * 768, 768)]
    lo = 0
    for width in (512, 512, 512, 512, 256, 256):
        rounds.append((W_D, lo, width))
        lo += width
    return rounds


def layer_kernel(rounds, x_loc, gain, cos_tab, sin_tab, keep, *refs):
    shards, refs = refs[:7], refs[7:]
    y_out, gathered, refs = refs[0], refs[1:8], refs[8:]
    (xg, act, big, mix, res, gbuf, wbuf, send_sem, recv_sem, x_send, x_recv, o_send, o_recv,
     g_send, g_recv, lsem, wsem, ysem) = refs
    mv = Mover(shards, gathered, rounds, send_sem, recv_sem)
    dx, fz, s = mv.dx, mv.fz, mv.s

    def at_rows(start, n):
        return pl.ds(pl.multiple_of(start, BLK), n)

    def x_copies():
        out = []
        for k in range(1, SP):
            t = lax.rem(s + k, SP)
            for b in range(PER):
                out.append(remote(x_loc.at[at_rows((PER * t + b) * BLK, BLK)], xg.at[at_rows(b * SEQ + s * BLK, BLK)],
                                  x_send.at[k - 1, b], x_recv.at[k - 1, b], (dx, fz, t)))
        return out

    def x_own():
        return [pltpu.make_async_copy(x_loc.at[at_rows((PER * s + b) * BLK, BLK)],
                                      xg.at[at_rows(b * SEQ + s * BLK, BLK)], lsem.at[b]) for b in range(PER)]

    def g_copies():
        return [remote(gain, gbuf.at[fz], g_send.at[k - 1], g_recv.at[k - 1], (dx, lax.rem(fz + k, NZ), s))
                for k in range(1, NZ)]

    def g_own():
        return pltpu.make_async_copy(gain, gbuf.at[fz], lsem.at[PER])

    def res_load():
        return pltpu.make_async_copy(x_loc, res, lsem.at[PER + 1])

    def o_copies(half):
        out = []
        cols = pl.ds(half * HALF, HALF)
        for k in range(1, SP):
            t = lax.rem(s + k, SP)
            for b in range(PER):
                out.append(remote(big.at[at_rows(b * SEQ + t * BLK, BLK), cols],
                                  mix.at[at_rows((PER * s + b) * BLK, BLK), cols],
                                  o_send.at[half, k - 1, b], o_recv.at[half, k - 1, b], (dx, fz, t)))
        return out

    def norm(src, row):
        gains = jnp.concatenate([gbuf[j, row:row + 1, :] for j in range(NZ)], axis=-1).astype(jnp.float32)

        def body(i, _):
            at = at_rows(i * BLK, BLK)
            h = src[at, :].astype(jnp.float32)
            inv = lax.rsqrt(jnp.mean(h * h, axis=-1, keepdims=True) + NORM_EPS)
            act[at, :] = (h * inv * gains).astype(jnp.bfloat16)
            return 0

        lax.fori_loop(0, TOK // BLK, body, 0)

    def loads(w, base, lo, slot, first):
        sh, g = shards[w], gathered[w]
        ks = sh.shape[0]
        cols = pl.ds(pl.multiple_of(lo, 128), TILE)
        out = []
        for j in range(NZ):
            src = sh.at[:, cols] if j == 0 else g.at[j, :, cols]
            at = pl.ds(pl.multiple_of(base + lax.rem(fz + j, NZ) * ks, 32), ks)
            out.append(pltpu.make_async_copy(src, wbuf.at[slot, at, :], wsem.at[slot, first + j]))
        return out

    def tiles(n, start, wait, compute):
        start(0, 0)

        def body(t, _):
            slot = lax.rem(t, 2)

            @pl.when(t + 1 < n)
            def _():
                start(t + 1, 1 - slot)

            wait(t, slot)
            compute(t, slot)
            return 0

        lax.fori_loop(0, n, body, 0)

    def simple(n, load, compute):
        def start(t, slot):
            for cp in load(t, slot):
                cp.start()

        def wait(t, slot):
            for cp in load(t, slot):
                cp.wait()

        tiles(n, start, wait, compute)

    m_rows = TOK // 2

    def by_rows(body):
        def go(m, _):
            body(pl.ds(pl.multiple_of(m * m_rows, m_rows), m_rows))
            return 0
        lax.fori_loop(0, TOK // m_rows, go, 0)

    def qkv(half):
        per = HALF // TILE

        def start(t, slot):
            for j, w in enumerate((W_Q, W_K, W_V)):
                @pl.when(lax.div(t, per) == j)
                def _():
                    for cp in loads(w, 0, half * HALF + lax.rem(t, per) * TILE, slot, 0):
                        cp.start()

        def wait(t, slot):
            for cp in loads(W_Q, 0, half * HALF + lax.rem(t, per) * TILE, slot, 0):
                cp.wait()

        def compute(t, slot):
            off = lax.div(t, per) * DIM + half * HALF + lax.rem(t, per) * TILE

            def body(at):
                acc = jnp.dot(act[at, :], wbuf[slot, 0:DIM, :], preferred_element_type=jnp.float32)

                @pl.when(t < 2 * per)
                def _():
                    cos, sin = cos_tab[at, :], sin_tab[at, :]
                    for h in range(TILE // HEAD_DIM):
                        p = acc[:, h * HEAD_DIM:(h + 1) * HEAD_DIM]
                        swapped = jnp.concatenate([p[:, HEAD_DIM // 2:], p[:, :HEAD_DIM // 2]], axis=-1)
                        rot = p * cos + swapped * sin
                        big[at, pl.ds(pl.multiple_of(off + h * HEAD_DIM, 128), HEAD_DIM)] = rot.astype(jnp.bfloat16)

                @pl.when(t >= 2 * per)
                def _():
                    big[at, pl.ds(pl.multiple_of(off, 128), TILE)] = acc.astype(jnp.bfloat16)

            by_rows(body)

        tiles(3 * per, start, wait, compute)

    def attention(half):
        n = HALF // HEAD_DIM

        def body(h, _):
            col = half * HALF + h * HEAD_DIM
            for b in range(PER):
                at = pl.ds(b * SEQ, SEQ)
                q, k, v = (big[at, pl.ds(pl.multiple_of(col + j * DIM, 128), HEAD_DIM)] for j in range(3))
                sc = lax.dot_general(q, k, (((1,), (1,)), ((), ())), preferred_element_type=jnp.float32)
                sc = jnp.where(keep[...] > 0, sc * HEAD_DIM ** -0.5, MASK_VALUE)
                e = jnp.exp(sc - jnp.max(sc, axis=-1, keepdims=True))
                tot = jnp.sum(e, axis=-1, keepdims=True)
                o = jnp.dot(e.astype(jnp.bfloat16), v, preferred_element_type=jnp.float32) / tot
                big[at, pl.ds(pl.multiple_of(col, 128), HEAD_DIM)] = o.astype(jnp.bfloat16)
            return 0

        lax.fori_loop(0, n, body, 0)

    def send_mix(half):
        for cp in o_copies(half):
            cp.start()
        cols = pl.ds(half * HALF, HALF)
        for b in range(PER):
            mix[at_rows((PER * s + b) * BLK, BLK), cols] = big[at_rows(b * SEQ + s * BLK, BLK), cols]

    def out_proj():
        for half in range(2):
            for cp in o_copies(half):
                cp.wait_recv()

        def load(t, slot):
            return loads(W_O, 0, t * TILE, slot, 0)

        def compute(t, slot):
            cols = pl.ds(pl.multiple_of(t * TILE, 128), TILE)

            def body(at):
                acc = jnp.dot(mix[at, :], wbuf[slot, 0:DIM, :], preferred_element_type=jnp.float32)
                res[at, cols] = (res[at, cols].astype(jnp.float32) + acc).astype(jnp.bfloat16)

            by_rows(body)

        simple(DIM // TILE, load, compute)
        norm(res, 1)
        for half in range(2):
            for cp in o_copies(half):
                cp.wait_send()

    def gate_up(lo, width):
        def load(t, slot):
            return loads(W_G, 0, lo + t * TILE, slot, 0) + loads(W_U, DIM, lo + t * TILE, slot, NZ)

        def compute(t, slot):
            def body(at):
                a = act[at, :]
                g = jnp.dot(a, wbuf[slot, 0:DIM, :], preferred_element_type=jnp.float32)
                u = jnp.dot(a, wbuf[slot, DIM:2 * DIM, :], preferred_element_type=jnp.float32)
                big[at, pl.ds(pl.multiple_of(lo + t * TILE, 128), TILE)] = (g / (1.0 + jnp.exp(-g)) * u).astype(jnp.bfloat16)

            by_rows(body)

        simple(width // TILE, load, compute)

    def y_copy(t):
        cols = pl.ds(pl.multiple_of(t * TILE, 128), TILE)
        return pltpu.make_async_copy(xg.at[:, cols], y_out.at[:, cols], ysem.at[t])

    def down(lo, width):
        def load(t, slot):
            return loads(W_D, 0, lo + t * TILE, slot, 0)

        def compute(t, slot):
            cols = pl.ds(pl.multiple_of(lo + t * TILE, 128), TILE)

            def body(at):
                acc = jnp.dot(big[at, 0:FFN], wbuf[slot, 0:FFN, :], preferred_element_type=jnp.float32)
                xg[at, cols] = (res[at, cols].astype(jnp.float32) + acc).astype(jnp.bfloat16)

            by_rows(body)
            y_copy(lo // TILE + t).start()

        simple(width // TILE, load, compute)

    def first_norm():
        for cp in x_copies() + g_copies():
            cp.wait_recv()
        for cp in x_own():
            cp.wait()
        g_own().wait()
        norm(xg, 0)

    def late_sends():
        for cp in x_copies() + g_copies():
            cp.wait_send()
        res_load().wait()

    for cp in x_copies() + g_copies() + x_own() + [g_own(), res_load()]:
        cp.start()
    hooks = {}

    def hook(tick, fn):
        hooks.setdefault(tick, []).append(fn)

    last = {}
    for r, (w, lo, width) in enumerate(rounds):
        last[(w, lo)] = r + LAG
    hook(3, first_norm)
    hook(4, late_sends)
    for half in range(2):
        tick = last[(W_V, half * HALF)]
        hook(tick, functools.partial(qkv, half))
        hook(tick + 1, functools.partial(attention, half))
        hook(tick + 1, functools.partial(send_mix, half))
    hook(max(last[(W_O, HALF)], last[(W_V, HALF)] + 2), out_proj)
    for w, lo, width in rounds:
        if w == W_U:
            hook(last[(w, lo)], functools.partial(gate_up, lo, width))
        if w == W_D:
            hook(last[(w, lo)], functools.partial(down, lo, width))
    for i in range(mv.ticks()):
        mv.step(i)
        for fn in hooks.get(i, ()):
            fn()
    for t in range(DIM // TILE):
        y_copy(t).wait()
    mv.finish()


def local_layer(x_loc, norm_attn, w_query, w_key, w_value, w_out, norm_mlp, w_gate, w_up, w_down):
    shards = (w_query, w_key, w_value, w_out, w_gate, w_up, w_down)
    gain = jnp.concatenate([norm_attn[None], norm_mlp[None], jnp.zeros((14, DIM // NZ), jnp.bfloat16)], axis=0)
    seq_idx = jnp.arange(SEQ, dtype=jnp.int32)
    pos = (seq_idx % BLK) * SP + seq_idx // BLK
    inv_freq = jnp.exp(jnp.arange(HEAD_DIM // 2, dtype=jnp.float32) * (-2.0 * math.log(ROPE_THETA) / HEAD_DIM))
    angles = pos.astype(jnp.float32)[:, None] * inv_freq[None, :]
    cos, sin = jnp.cos(angles), jnp.sin(angles)
    cos_tab = jnp.tile(jnp.concatenate([cos, cos], axis=-1), (PER, 1))
    sin_tab = jnp.tile(jnp.concatenate([-sin, sin], axis=-1), (PER, 1))
    keep = (pos[None, :] <= pos[:, None]).astype(jnp.float32)
    rounds = plan()
    any_spec = pl.BlockSpec(memory_space=pl.ANY)
    vmem_spec = pl.BlockSpec(memory_space=pltpu.VMEM)
    dma = pltpu.SemaphoreType.DMA
    bf16 = jnp.bfloat16
    outs = [jax.ShapeDtypeStruct((TOK, DIM), bf16)]
    outs += [jax.ShapeDtypeStruct((NZ,) + w.shape, bf16) for w in shards]
    res = pl.pallas_call(
        functools.partial(layer_kernel, rounds),
        out_shape=outs,
        in_specs=[any_spec, any_spec] + [vmem_spec] * 3 + [any_spec] * 7,
        out_specs=[any_spec] * 8,
        scratch_shapes=[
            pltpu.VMEM((TOK, DIM), bf16), pltpu.VMEM((TOK, DIM), bf16), pltpu.VMEM((TOK, 3 * DIM), bf16),
            pltpu.VMEM((TOK, DIM), bf16), pltpu.VMEM((TOK, DIM), bf16), pltpu.VMEM((NZ, 16, DIM // NZ), bf16),
            pltpu.VMEM((2, FFN, TILE), bf16),
            dma((SLOTS, N_KINDS)), dma((SLOTS, N_KINDS)), dma((SP - 1, PER)), dma((SP - 1, PER)),
            dma((2, SP - 1, PER)), dma((2, SP - 1, PER)), dma((NZ - 1,)), dma((NZ - 1,)),
            dma((PER + 2,)), dma((2, 2 * NZ)), dma((DIM // TILE,))],
        compiler_params=pltpu.CompilerParams(has_side_effects=True, vmem_limit_bytes=60 * 1024 * 1024),
    )(x_loc.reshape(TOK, DIM), gain, cos_tab, sin_tab, keep, *shards)
    return res[0].reshape(x_loc.shape)


def solution(mesh):
    row_spec = P(('dp', 'fsdp'), 'sp', None)
    weight_spec = P('fsdp', None)
    gain_spec = P('fsdp')
    in_specs = (row_spec, gain_spec, weight_spec, weight_spec, weight_spec, weight_spec, gain_spec, weight_spec, weight_spec, weight_spec)
    return jax.shard_map(local_layer, mesh=mesh, in_specs=in_specs, out_specs=row_spec, check_vma=False)
```

```python
import math
import functools
import jax
import jax.numpy as jnp
from jax import lax
from jax.experimental import pallas as pl
from jax.experimental.pallas import tpu as pltpu
from jax.sharding import PartitionSpec as P

HEAD_DIM = 128
NORM_EPS = 1e-5
ROPE_THETA = 5e7
MASK_VALUE = -1e30
MESH = pl.DeviceIdType.MESH
NZ = 4
SP = 4
ROWS = 12
BLK = 64
SEQ = SP * BLK
TOK = ROWS * BLK
ALL = ROWS * SEQ
DIM = 2560
FFN = 6912
HALF = DIM // 2
OWN = DIM // SP
HEADS = OWN // 128
PARTS = 3
OUT_WAIT = 1
EARLY = 13
FORWARD_TICKS = (2, 4, 6, 7)
GATE_WIDTHS = (1536, 1536, 1280, 1280, 768, 512)
DOWN_WIDTHS = (768, 768, 512, 256, 256)
TILE = 256
N_KINDS = 16
SLOTS = 12
AHEAD = 3
LAG = 5
Z_STAGES = ('z1', 'z2', 'z3')
W_Q, W_K, W_V, W_O, W_G, W_U, W_D = range(7)


def split_rows(block, early):
    if early:
        over_z = block // 16 * 8
        return over_z, block - over_z
    over_z = block // 24 * 8
    return over_z, (block - over_z) // 16 * 8 + (8 if block % 24 else 0)


def remote(src, dst, send_sem, recv_sem, dev):
    return pltpu.make_async_remote_copy(
        src_ref=src, dst_ref=dst, send_sem=send_sem, recv_sem=recv_sem, device_id=dev, device_id_type=MESH)


class Mover:
    def __init__(self, shards, gathered, rounds, early, send_sem, recv_sem):
        self.early = early
        self.shards, self.gathered, self.rounds = shards, gathered, rounds
        self.send_sem, self.recv_sem = send_sem, recv_sem
        dx, fz, s = lax.axis_index('dp'), lax.axis_index('fsdp'), lax.axis_index('sp')
        self.dx, self.fz, self.s = dx, fz, s
        self.y, self.c = lax.div(s, 2), lax.rem(s, 2)
        self.core_dev = (dx, fz, self.y * 2 + (1 - self.c))
        self.x_dev = (1 - dx, fz, s)
        self.y_dev = (dx, fz, (1 - self.y) * 2 + self.c)

    def block(self, dx, y, c):
        return (dx * 2 + y) * 2 + c

    def copies(self, r, stage):
        w, lo, width = self.rounds[r]
        sh, g = self.shards[w], self.gathered[w]
        rb = sh.shape[0] // 8
        cols = pl.ds(lo, width)
        az, ax = split_rows(rb, r < self.early)
        dx, y, c = self.dx, self.y, self.c
        mine = self.block(dx, y, c)
        diag = self.block(1 - dx, 1 - y, c)
        xblk, yblk = self.block(1 - dx, y, c), self.block(dx, 1 - y, c)
        slot = r % SLOTS
        out = []

        def rows(blk, a, b):
            return pl.ds(pl.multiple_of(blk * rb + a, 8), b - a)

        def add(kind, src, dst, dev):
            out.append(remote(src, dst, self.send_sem.at[slot, kind], self.recv_sem.at[slot, kind], dev))

        def same(kind, blk, a, b, dev):
            if a == b:
                return
            ref = g.at[1:NZ, rows(blk, a, b), cols]
            add(kind, ref, ref, dev)

        if w <= W_V:
            at = pl.ds(pl.multiple_of(dx * (DIM // 8), 8), DIM // 8)
            cols = pl.ds(pl.multiple_of(self.s * OWN + lo, 128), width)
            if stage in Z_STAGES:
                k = int(stage[1])
                add(k - 1, sh.at[at, cols], g.at[NZ - k, at, cols], (dx, lax.rem(self.fz + k, NZ), self.s))
            if stage == 'zf':
                low = self.fz < NZ // 2
                add(14, g.at[2, at, cols], g.at[jnp.where(low, NZ - 1, 1), at, cols],
                    (dx, jnp.where(low, 0, NZ - 1), self.s))
            if stage == 'p1':
                ref = g.at[1:NZ, at, cols]
                add(6, ref, ref, self.x_dev)
            return out
        if stage in Z_STAGES:
            k = int(stage[1])
            dev = (dx, lax.rem(self.fz + k, NZ), self.s)
            add(k - 1, sh.at[rows(mine, 0, rb), cols], g.at[NZ - k, rows(mine, 0, rb), cols], dev)
            add(k + 2, sh.at[rows(diag, 0, az), cols], g.at[NZ - k, rows(diag, 0, az), cols], dev)
        if stage == 'zf':
            low = self.fz < NZ // 2
            dev = (dx, jnp.where(low, 0, NZ - 1), self.s)
            there = jnp.where(low, NZ - 1, 1)
            for kind, blk, top in ((14, mine, rb), (15, diag, az)):
                add(kind, g.at[2, rows(blk, 0, top), cols], g.at[there, rows(blk, 0, top), cols], dev)
        if stage == 'p1':
            same(6, mine, 0, rb, self.x_dev)
            same(7, mine, 0, rb, self.y_dev)
        if stage == 'p1c':
            same(8, mine, 0, rb, self.core_dev)
        if stage == 'p2':
            same(9, yblk, az, az + ax, self.x_dev)
            same(10, xblk, az + ax, rb, self.y_dev)
        if stage == 'p2c':
            same(11, xblk, 0, rb, self.core_dev)
            same(12, yblk, 0, rb, self.core_dev)
        if stage == 'p3':
            same(13, diag, 0, rb, self.core_dev)
        return out

    def when_send(self, stage):
        if stage == 'z1':
            return self.fz != NZ - 1
        if stage == 'z3':
            return self.fz != 0
        if stage == 'zf':
            return jnp.logical_and(self.fz != 0, self.fz != NZ - 1)
        return None

    def when_recv(self, stage):
        if stage == 'z1':
            return self.fz != 0
        if stage == 'z3':
            return self.fz != NZ - 1
        if stage == 'zf':
            return jnp.logical_or(self.fz == 0, self.fz == NZ - 1)
        return None

    def each(self, r, stages, when, act):
        if 0 <= r < len(self.rounds):
            for stage in stages:
                cond = when(stage)

                def go():
                    for cp in self.copies(r, stage):
                        act(cp)

                if cond is None:
                    go()
                else:
                    pl.when(cond)(go)

    def start(self, r, *stages):
        self.each(r, stages, self.when_send, lambda cp: cp.start())

    def wait_recv(self, r, *stages):
        self.each(r, stages, self.when_recv, lambda cp: cp.wait_recv())

    def wait_send(self, r):
        self.each(r, Z_STAGES + ('zf', 'p1', 'p1c', 'p2', 'p2c', 'p3'), self.when_send, lambda cp: cp.wait_send())

    def step(self, i):
        if i == 0:
            for r in range(AHEAD):
                self.start(r, *Z_STAGES)
        self.wait_send(i + AHEAD - SLOTS)
        self.start(i + AHEAD, *Z_STAGES)
        self.wait_recv(i, *Z_STAGES)
        self.start(i, 'zf')
        self.wait_recv(i, 'zf')
        self.start(i, 'p1', 'p1c')
        self.wait_recv(i - 2, 'p1')
        self.start(i - 2, 'p2', 'p2c')
        self.wait_recv(i - 4, 'p2')
        self.start(i - 4, 'p3')
        self.wait_recv(i - 5, 'p1c', 'p2c', 'p3')

    def ticks(self):
        return len(self.rounds) + LAG

    def finish(self):
        n = len(self.rounds)
        done = n + LAG + AHEAD - SLOTS
        for r in range(max(done, 0), n):
            self.wait_send(r)


def plan():
    rounds = []

    def add(weights, widths):
        lo = 0
        for width in widths:
            rounds.extend((w, lo, width) for w in weights)
            lo += width

    add((W_Q,), (128, 256, 256))
    add((W_K,), (256, 384))
    add((W_V,), (256, 384))
    add((W_O,), (HALF, HALF))
    add((W_G, W_U), GATE_WIDTHS)
    add((W_D,), DOWN_WIDTHS)
    return rounds, EARLY


def layer_kernel(rounds, early, x_loc, gain, cos_tab, sin_tab, keep, *refs):
    shards, refs = refs[:7], refs[7:]
    y_out, gathered, refs = refs[0], refs[1:8], refs[8:]
    (xa, big, mix, res, gbuf, wbuf, send_sem, recv_sem, x_send, x_recv, o_send, o_recv,
     g_send, g_recv, lsem, wsem, ysem) = refs
    mv = Mover(shards, gathered, rounds, early, send_sem, recv_sem)
    dx, fz, s = mv.dx, mv.fz, mv.s
    s_y = (1 - mv.y) * 2 + mv.c
    per = ROWS // PARTS

    def at_rows(start, n):
        return pl.ds(pl.multiple_of(start, BLK), n)

    def for_each(lo, hi, body):
        def go(b, _):
            body(b)
            return 0
        lax.fori_loop(lo, hi, go, 0)

    def x_copy(k, b):
        mine, theirs = at_rows(b * SEQ + s * BLK, BLK), at_rows(b * SEQ + s_y * BLK, BLK)
        here = x_loc.at[at_rows(b * BLK, BLK)]
        src, dst, dev = ((here, xa.at[mine], mv.y_dev), (here, xa.at[mine], mv.core_dev),
                         (xa.at[theirs], xa.at[theirs], mv.core_dev))[k]
        return remote(src, dst, x_send.at[k, b], x_recv.at[k, b], dev)

    def x_own(b):
        return pltpu.make_async_copy(x_loc.at[at_rows(b * BLK, BLK)], xa.at[at_rows(b * SEQ + s * BLK, BLK)], lsem.at[b])

    def g_copies():
        return [remote(gain, gbuf.at[fz], g_send.at[k - 1], g_recv.at[k - 1], (dx, lax.rem(fz + k, NZ), s))
                for k in range(1, NZ)]

    def g_own():
        return pltpu.make_async_copy(gain, gbuf.at[fz], lsem.at[ROWS])

    def res_load():
        return pltpu.make_async_copy(x_loc, res, lsem.at[ROWS + 1])

    def o_copy(k, b):
        t = lax.rem(s + k, SP)
        return remote(big.at[at_rows(b * SEQ + t * BLK, BLK), 0:OWN],
                      mix.at[at_rows(b * BLK, BLK), pl.ds(pl.multiple_of(s * OWN, 128), OWN)],
                      o_send.at[k - 1, b], o_recv.at[k - 1, b], (dx, fz, t))

    def x_forward(lo, hi):
        def body(b):
            x_copy(0, b).wait_recv()
            x_copy(2, b).start()
        for_each(lo, hi, body)

    def norm(src, dst, row, lo, n):
        gains = jnp.concatenate([gbuf[j, row:row + 1, :] for j in range(NZ)], axis=-1).astype(jnp.float32)

        def body(i):
            h = src[at_rows(lo + i * BLK, BLK), :].astype(jnp.float32)
            inv = lax.rsqrt(jnp.mean(h * h, axis=-1, keepdims=True) + NORM_EPS)
            dst(i)[...] = (h * inv * gains).astype(jnp.bfloat16)

        for_each(0, n // BLK, body)

    def x_norm(part):
        if part == 0:
            for cp in g_copies():
                cp.wait_recv()
            g_own().wait()

        def body(b):
            x_copy(1, b).wait_recv()
            x_copy(2, b).wait_recv()
            x_copy(2, b).wait_send()
            x_own(b).wait()

        for_each(part * per, part * per + per, body)
        lo = part * per * SEQ
        norm(xa, lambda i: xa.at[at_rows(lo + i * BLK, BLK)], 0, lo, per * SEQ)

    def late_sends():
        def body(b):
            for k in range(2):
                x_copy(k, b).wait_send()
        for_each(0, ROWS, body)
        for cp in g_copies():
            cp.wait_send()
        res_load().wait()

    def piece(w, base, lo, width, slot, first, col):
        sh, g = shards[w], gathered[w]
        ks = sh.shape[0]
        cols = pl.ds(pl.multiple_of(lo, 128), width)
        out = []
        for j in range(NZ):
            src = sh.at[:, cols] if j == 0 else g.at[j, :, cols]
            at = pl.ds(pl.multiple_of(base + lax.rem(fz + j, NZ) * ks, 32), ks)
            out.append(pltpu.make_async_copy(src, wbuf.at[slot, at, col:col + width], wsem.at[slot, first + j]))
        return out

    def tiles(n, start, wait, compute):
        start(0, 0)

        def body(t):
            slot = lax.rem(t, 2)

            @pl.when(t + 1 < n)
            def _():
                start(t + 1, 1 - slot)

            wait(t, slot)
            compute(t, slot)

        for_each(0, n, body)

    def simple(n, load, compute):
        def start(t, slot):
            for cp in load(t, slot):
                cp.start()

        def wait(t, slot):
            for cp in load(t, slot):
                cp.wait()

        tiles(n, start, wait, compute)

    def by_rows(n, rows, body):
        for_each(0, n, lambda m: body(pl.ds(pl.multiple_of(m * rows, rows), rows)))

    m_rows = TOK // 2
    n_m = TOK // m_rows

    def qkv(part):
        rows = 2 * SEQ
        top = 3 * HEADS - 1

        def start(t, slot):
            for side in range(2):
                hh = jnp.minimum(2 * t + side, top)
                for j, w in enumerate((W_Q, W_K, W_V)):
                    @pl.when(lax.div(hh, HEADS) == j)
                    def _():
                        for cp in piece(w, 0, s * OWN + lax.rem(hh, HEADS) * 128, 128, slot, NZ * side, 128 * side):
                            cp.start()

        def wait(t, slot):
            for side in range(2):
                for cp in piece(W_Q, 0, s * OWN, 128, slot, NZ * side, 128 * side):
                    cp.wait()

        def compute(t, slot):
            def body(m):
                at = at_rows(part * per * SEQ + m * rows, rows)
                acc = jnp.dot(xa[at, :], wbuf[slot, 0:DIM, :], preferred_element_type=jnp.float32)
                cos, sin = cos_tab[...], sin_tab[...]
                for side in range(2):
                    p = acc[:, side * 128:(side + 1) * 128]
                    swapped = jnp.concatenate([p[:, 64:], p[:, :64]], axis=-1)
                    turned = 2 * t + side < 2 * HEADS
                    val = jnp.where(turned, p * cos + swapped * sin, p)
                    big[at, pl.ds(pl.multiple_of((2 * t + side) * 128, 128), 128)] = val.astype(jnp.bfloat16)

            for_each(0, per * SEQ // rows, body)

        tiles(8, start, wait, compute)

    def attention(part):
        def body(b):
            at = at_rows(b * SEQ, SEQ)
            for h in range(HEADS):
                q, k, v = (big[at, (j * HEADS + h) * 128:(j * HEADS + h + 1) * 128] for j in range(3))
                sc = lax.dot_general(q, k, (((1,), (1,)), ((), ())), preferred_element_type=jnp.float32)
                sc = jnp.where(keep[...] > 0, sc * HEAD_DIM ** -0.5, MASK_VALUE)
                e = jnp.exp(sc - jnp.max(sc, axis=-1, keepdims=True))
                tot = jnp.sum(e, axis=-1, keepdims=True)
                o = jnp.dot(e.astype(jnp.bfloat16), v, preferred_element_type=jnp.float32) / tot
                big[at, h * 128:(h + 1) * 128] = o.astype(jnp.bfloat16)

        for_each(part * per, part * per + per, body)

    def send_mix(part):
        def body(b):
            for k in range(1, SP):
                o_copy(k, b).start()
            mix[at_rows(b * BLK, BLK), pl.ds(pl.multiple_of(s * OWN, 128), OWN)] = big[at_rows(b * SEQ + s * BLK, BLK), 0:OWN]

        for_each(part * per, part * per + per, body)

    act_at = 3 * TOK

    def out_proj():
        def arrive(b):
            for k in range(1, SP):
                o_copy(k, b).wait_recv()
        for_each(0, ROWS, arrive)

        def load(t, slot):
            return piece(W_O, 0, t * TILE, TILE, slot, 0, 0)

        def compute(t, slot):
            cols = pl.ds(pl.multiple_of(t * TILE, 128), TILE)

            def body(at):
                acc = jnp.dot(mix[at, :], wbuf[slot, 0:DIM, :], preferred_element_type=jnp.float32)
                res[at, cols] = (res[at, cols].astype(jnp.float32) + acc).astype(jnp.bfloat16)

            by_rows(n_m, m_rows, body)

        simple(DIM // TILE, load, compute)
        norm(res, lambda i: xa.at[at_rows(act_at + i * BLK, BLK)], 1, 0, TOK)

        def gone(b):
            for k in range(1, SP):
                o_copy(k, b).wait_send()
        for_each(0, ROWS, gone)

    def gate_up(lo, width):
        def load(t, slot):
            return (piece(W_G, 0, lo + t * TILE, TILE, slot, 0, 0)
                    + piece(W_U, DIM, lo + t * TILE, TILE, slot, NZ, 0))

        def compute(t, slot):
            tile = lo // TILE + t
            blk = lax.div(tile, DIM // TILE)
            cols = pl.ds(pl.multiple_of(lax.rem(tile, DIM // TILE) * TILE, 128), TILE)

            def body(m):
                a = xa[pl.ds(pl.multiple_of(act_at + m * m_rows, m_rows), m_rows), :]
                g = jnp.dot(a, wbuf[slot, 0:DIM, :], preferred_element_type=jnp.float32)
                u = jnp.dot(a, wbuf[slot, DIM:2 * DIM, :], preferred_element_type=jnp.float32)
                at = pl.ds(pl.multiple_of(blk * TOK + m * m_rows, m_rows), m_rows)
                xa[at, cols] = (g / (1.0 + jnp.exp(-g)) * u).astype(jnp.bfloat16)

            for_each(0, n_m, body)

        simple(width // TILE, load, compute)

    def y_copy(t):
        cols = pl.ds(pl.multiple_of(t * TILE, 128), TILE)
        return pltpu.make_async_copy(mix.at[:, cols], y_out.at[:, cols], ysem.at[t])

    def down(lo, width):
        def load(t, slot):
            return piece(W_D, 0, lo + t * TILE, TILE, slot, 0, 0)

        def compute(t, slot):
            cols = pl.ds(pl.multiple_of(lo + t * TILE, 128), TILE)

            def body(m):
                acc = None
                for j in range(3):
                    n = min(DIM, FFN - j * DIM)
                    h = xa[pl.ds(pl.multiple_of(j * TOK + m * m_rows, m_rows), m_rows), 0:n]
                    d = jnp.dot(h, wbuf[slot, j * DIM:j * DIM + n, :], preferred_element_type=jnp.float32)
                    acc = d if acc is None else acc + d
                at = pl.ds(pl.multiple_of(m * m_rows, m_rows), m_rows)
                mix[at, cols] = (res[at, cols].astype(jnp.float32) + acc).astype(jnp.bfloat16)

            for_each(0, n_m, body)
            y_copy(lo // TILE + t).start()

        simple(width // TILE, load, compute)

    def begin(b):
        x_copy(0, b).start()
        x_copy(1, b).start()
        x_own(b).start()

    for cp in g_copies() + [g_own()]:
        cp.start()
    for_each(0, ROWS, begin)
    res_load().start()
    hooks = {}

    def hook(tick, fn, *args):
        hooks.setdefault(tick, []).append(functools.partial(fn, *args))

    last = {}
    for r, (w, lo, width) in enumerate(rounds):
        last[(w, lo)] = r + (2 if w <= W_V else LAG)
    for j, tick in enumerate(FORWARD_TICKS):
        hook(tick, x_forward, 3 * j, 3 * j + 3)
    tick = last[(W_V, 256)]
    for part in range(PARTS):
        hook(tick - 2 + part, x_norm, part)
    hook(tick, late_sends)
    for part in range(PARTS):
        hook(tick + part, qkv, part)
        hook(tick + part, attention, part)
        hook(tick + part, send_mix, part)
    tick = max(last[(W_O, HALF)], tick + PARTS + OUT_WAIT)
    hook(tick, out_proj)
    for w, lo, width in rounds:
        if w == W_U:
            tick = max(tick + 1, last[(w, lo)])
            hook(tick, gate_up, lo, width)
        if w == W_D:
            hook(last[(w, lo)], down, lo, width)
    for i in range(mv.ticks()):
        mv.step(i)
        for fn in hooks.get(i, ()):
            fn()
    for t in range(DIM // TILE):
        y_copy(t).wait()
    mv.finish()


def local_layer(x_loc, norm_attn, w_query, w_key, w_value, w_out, norm_mlp, w_gate, w_up, w_down):
    shards = (w_query, w_key, w_value, w_out, w_gate, w_up, w_down)
    gain = jnp.concatenate([norm_attn[None], norm_mlp[None], jnp.zeros((14, DIM // NZ), jnp.bfloat16)], axis=0)
    seq_idx = jnp.arange(SEQ, dtype=jnp.int32)
    pos = (seq_idx % BLK) * SP + seq_idx // BLK
    inv_freq = jnp.exp(jnp.arange(HEAD_DIM // 2, dtype=jnp.float32) * (-2.0 * math.log(ROPE_THETA) / HEAD_DIM))
    angles = pos.astype(jnp.float32)[:, None] * inv_freq[None, :]
    cos, sin = jnp.cos(angles), jnp.sin(angles)
    cos_tab = jnp.tile(jnp.concatenate([cos, cos], axis=-1), (2, 1))
    sin_tab = jnp.tile(jnp.concatenate([-sin, sin], axis=-1), (2, 1))
    keep = (pos[None, :] <= pos[:, None]).astype(jnp.float32)
    rounds, early = plan()
    any_spec = pl.BlockSpec(memory_space=pl.ANY)
    vmem_spec = pl.BlockSpec(memory_space=pltpu.VMEM)
    dma = pltpu.SemaphoreType.DMA
    bf16 = jnp.bfloat16
    outs = [jax.ShapeDtypeStruct((TOK, DIM), bf16)]
    outs += [jax.ShapeDtypeStruct((NZ,) + w.shape, bf16) for w in shards]
    res = pl.pallas_call(
        functools.partial(layer_kernel, rounds, early),
        out_shape=outs,
        in_specs=[any_spec, any_spec] + [vmem_spec] * 3 + [any_spec] * 7,
        out_specs=[any_spec] * 8,
        scratch_shapes=[
            pltpu.VMEM((ALL, DIM), bf16), pltpu.VMEM((ALL, 16 * 128), bf16), pltpu.VMEM((TOK, DIM), bf16),
            pltpu.VMEM((TOK, DIM), bf16), pltpu.VMEM((NZ, 16, DIM // NZ), bf16), pltpu.VMEM((2, FFN, TILE), bf16),
            dma((SLOTS, N_KINDS)), dma((SLOTS, N_KINDS)), dma((3, ROWS)), dma((3, ROWS)),
            dma((SP - 1, ROWS)), dma((SP - 1, ROWS)), dma((NZ - 1,)), dma((NZ - 1,)),
            dma((ROWS + 2,)), dma((2, 2 * NZ)), dma((DIM // TILE,))],
        compiler_params=pltpu.CompilerParams(has_side_effects=True, vmem_limit_bytes=60 * 1024 * 1024),
    )(x_loc.reshape(TOK, DIM), gain, cos_tab, sin_tab, keep, *shards)
    return res[0].reshape(x_loc.shape)


def solution(mesh):
    row_spec = P(('dp', 'fsdp'), 'sp', None)
    weight_spec = P('fsdp', None)
    gain_spec = P('fsdp')
    in_specs = (row_spec, gain_spec, weight_spec, weight_spec, weight_spec, weight_spec, gain_spec, weight_spec, weight_spec, weight_spec)
    return jax.shard_map(local_layer, mesh=mesh, in_specs=in_specs, out_specs=row_spec, check_vma=False)
```

```python
import math
import functools
import jax
import jax.numpy as jnp
from jax import lax
from jax.experimental import pallas as pl
from jax.experimental.pallas import tpu as pltpu
from jax.sharding import PartitionSpec as P

HEAD_DIM = 128
NORM_EPS = 1e-5
ROPE_THETA = 5e7
MASK_VALUE = -1e30
MESH = pl.DeviceIdType.MESH
NZ = 4
SP = 4
ROWS = 12
BLK = 64
SEQ = SP * BLK
TOK = ROWS * BLK
ALL = ROWS * SEQ
DIM = 2560
FFN = 6912
HALF = DIM // 2
OWN = DIM // SP
HEADS = OWN // 128
PARTS = 3
OUT_WAIT = 1
EARLY = 11
FORWARD_TICKS = (2, 4, 6, 7)
GATE_WIDTHS = (1536, 1536, 1280, 1280, 768, 512)
DOWN_WIDTHS = (512, 512, 256, 256, 256, 256, 256, 256)
TILE = 256
N_KINDS = 16
SLOTS = 12
AHEAD = 2
LAG = 5
Z_STAGES = ('z1', 'z2', 'z3')
W_Q, W_K, W_V, W_O, W_G, W_U, W_D = range(7)


def split_rows(block, early):
    if early:
        over_z = block // 16 * 8
        return over_z, block - over_z
    over_z = block // 24 * 8
    return over_z, (block - over_z) // 16 * 8 + (8 if block % 24 else 0)


def remote(src, dst, send_sem, recv_sem, dev):
    return pltpu.make_async_remote_copy(
        src_ref=src, dst_ref=dst, send_sem=send_sem, recv_sem=recv_sem, device_id=dev, device_id_type=MESH)


class Mover:
    def __init__(self, shards, gathered, rounds, early, send_sem, recv_sem):
        self.early = early
        self.shards, self.gathered, self.rounds = shards, gathered, rounds
        self.send_sem, self.recv_sem = send_sem, recv_sem
        dx, fz, s = lax.axis_index('dp'), lax.axis_index('fsdp'), lax.axis_index('sp')
        self.dx, self.fz, self.s = dx, fz, s
        self.y, self.c = lax.div(s, 2), lax.rem(s, 2)
        self.core_dev = (dx, fz, self.y * 2 + (1 - self.c))
        self.x_dev = (1 - dx, fz, s)
        self.y_dev = (dx, fz, (1 - self.y) * 2 + self.c)

    def block(self, dx, y, c):
        return (dx * 2 + y) * 2 + c

    def copies(self, r, stage):
        w, lo, width = self.rounds[r]
        sh, g = self.shards[w], self.gathered[w]
        rb = sh.shape[0] // 8
        cols = pl.ds(lo, width)
        az, ax = split_rows(rb, r < self.early)
        dx, y, c = self.dx, self.y, self.c
        mine = self.block(dx, y, c)
        diag = self.block(1 - dx, 1 - y, c)
        xblk, yblk = self.block(1 - dx, y, c), self.block(dx, 1 - y, c)
        slot = r % SLOTS
        out = []

        def rows(blk, a, b):
            return pl.ds(pl.multiple_of(blk * rb + a, 8), b - a)

        def add(kind, src, dst, dev):
            out.append(remote(src, dst, self.send_sem.at[slot, kind], self.recv_sem.at[slot, kind], dev))

        def same(kind, blk, a, b, dev):
            if a == b:
                return
            ref = g.at[1:NZ, rows(blk, a, b), cols]
            add(kind, ref, ref, dev)

        if w <= W_V:
            at = pl.ds(pl.multiple_of(dx * (DIM // 8), 8), DIM // 8)
            cols = pl.ds(pl.multiple_of(self.s * OWN + lo, 128), width)
            if stage in Z_STAGES:
                k = int(stage[1])
                add(k - 1, sh.at[at, cols], g.at[NZ - k, at, cols], (dx, lax.rem(self.fz + k, NZ), self.s))
            if stage == 'zf':
                low = self.fz < NZ // 2
                add(14, g.at[2, at, cols], g.at[jnp.where(low, NZ - 1, 1), at, cols],
                    (dx, jnp.where(low, 0, NZ - 1), self.s))
            if stage == 'p1':
                ref = g.at[1:NZ, at, cols]
                add(6, ref, ref, self.x_dev)
            return out
        if stage in Z_STAGES:
            k = int(stage[1])
            dev = (dx, lax.rem(self.fz + k, NZ), self.s)
            add(k - 1, sh.at[rows(mine, 0, rb), cols], g.at[NZ - k, rows(mine, 0, rb), cols], dev)
            add(k + 2, sh.at[rows(diag, 0, az), cols], g.at[NZ - k, rows(diag, 0, az), cols], dev)
        if stage == 'zf':
            low = self.fz < NZ // 2
            dev = (dx, jnp.where(low, 0, NZ - 1), self.s)
            there = jnp.where(low, NZ - 1, 1)
            for kind, blk, top in ((14, mine, rb), (15, diag, az)):
                add(kind, g.at[2, rows(blk, 0, top), cols], g.at[there, rows(blk, 0, top), cols], dev)
        if stage == 'p1':
            same(6, mine, 0, rb, self.x_dev)
            same(7, mine, 0, rb, self.y_dev)
        if stage == 'p1c':
            same(8, mine, 0, rb, self.core_dev)
        if stage == 'p2':
            same(9, yblk, az, az + ax, self.x_dev)
            same(10, xblk, az + ax, rb, self.y_dev)
        if stage == 'p2c':
            same(11, xblk, 0, rb, self.core_dev)
            same(12, yblk, 0, rb, self.core_dev)
        if stage == 'p3':
            same(13, diag, 0, rb, self.core_dev)
        return out

    def when_send(self, stage):
        if stage == 'z1':
            return self.fz != NZ - 1
        if stage == 'z3':
            return self.fz != 0
        if stage == 'zf':
            return jnp.logical_and(self.fz != 0, self.fz != NZ - 1)
        return None

    def when_recv(self, stage):
        if stage == 'z1':
            return self.fz != 0
        if stage == 'z3':
            return self.fz != NZ - 1
        if stage == 'zf':
            return jnp.logical_or(self.fz == 0, self.fz == NZ - 1)
        return None

    def each(self, r, stages, when, act):
        if 0 <= r < len(self.rounds):
            for stage in stages:
                cond = when(stage)

                def go():
                    for cp in self.copies(r, stage):
                        act(cp)

                if cond is None:
                    go()
                else:
                    pl.when(cond)(go)

    def start(self, r, *stages):
        self.each(r, stages, self.when_send, lambda cp: cp.start())

    def wait_recv(self, r, *stages):
        self.each(r, stages, self.when_recv, lambda cp: cp.wait_recv())

    def wait_send(self, r):
        self.each(r, Z_STAGES + ('zf', 'p1', 'p1c', 'p2', 'p2c', 'p3'), self.when_send, lambda cp: cp.wait_send())

    def step(self, i):
        if i == 0:
            for r in range(AHEAD):
                self.start(r, *Z_STAGES)
        self.wait_send(i + AHEAD - SLOTS)
        self.start(i + AHEAD, *Z_STAGES)
        self.wait_recv(i, *Z_STAGES)
        self.start(i, 'zf')
        self.wait_recv(i, 'zf')
        self.start(i, 'p1', 'p1c')
        self.wait_recv(i - 2, 'p1')
        self.start(i - 2, 'p2', 'p2c')
        self.wait_recv(i - 4, 'p2')
        self.start(i - 4, 'p3')
        self.wait_recv(i - 5, 'p1c', 'p2c', 'p3')

    def ticks(self):
        return len(self.rounds) + LAG

    def finish(self):
        n = len(self.rounds)
        done = n + LAG + AHEAD - SLOTS
        for r in range(max(done, 0), n):
            self.wait_send(r)


def plan():
    rounds = []

    def add(weights, widths):
        lo = 0
        for width in widths:
            rounds.extend((w, lo, width) for w in weights)
            lo += width

    add((W_Q,), (128, 256, 256))
    add((W_K,), (256, 384))
    add((W_V,), (256, 384))
    add((W_O,), (HALF, HALF))
    add((W_G, W_U), GATE_WIDTHS)
    add((W_D,), DOWN_WIDTHS)
    return rounds, EARLY


def layer_kernel(rounds, early, x_loc, gain, cos_tab, sin_tab, keep, *refs):
    shards, refs = refs[:7], refs[7:]
    y_out, gathered, refs = refs[0], refs[1:8], refs[8:]
    (xa, big, mix, res, gbuf, wbuf, send_sem, recv_sem, x_send, x_recv, o_send, o_recv,
     g_send, g_recv, lsem, wsem, ysem) = refs
    mv = Mover(shards, gathered, rounds, early, send_sem, recv_sem)
    dx, fz, s = mv.dx, mv.fz, mv.s
    s_y = (1 - mv.y) * 2 + mv.c
    per = ROWS // PARTS

    def at_rows(start, n):
        return pl.ds(pl.multiple_of(start, BLK), n)

    def for_each(lo, hi, body):
        def go(b, _):
            body(b)
            return 0
        lax.fori_loop(lo, hi, go, 0)

    def x_copy(k, b):
        mine, theirs = at_rows(b * SEQ + s * BLK, BLK), at_rows(b * SEQ + s_y * BLK, BLK)
        here = x_loc.at[at_rows(b * BLK, BLK)]
        src, dst, dev = ((here, xa.at[mine], mv.y_dev), (here, xa.at[mine], mv.core_dev),
                         (xa.at[theirs], xa.at[theirs], mv.core_dev))[k]
        return remote(src, dst, x_send.at[k, b], x_recv.at[k, b], dev)

    def x_own(b):
        return pltpu.make_async_copy(x_loc.at[at_rows(b * BLK, BLK)], xa.at[at_rows(b * SEQ + s * BLK, BLK)], lsem.at[b])

    def g_copies():
        return [remote(gain, gbuf.at[fz], g_send.at[k - 1], g_recv.at[k - 1], (dx, lax.rem(fz + k, NZ), s))
                for k in range(1, NZ)]

    def g_own():
        return pltpu.make_async_copy(gain, gbuf.at[fz], lsem.at[ROWS])

    def res_load():
        return pltpu.make_async_copy(x_loc, res, lsem.at[ROWS + 1])

    def o_copy(k, b):
        t = lax.rem(s + k, SP)
        return remote(big.at[at_rows(b * SEQ + t * BLK, BLK), 0:OWN],
                      mix.at[at_rows(b * BLK, BLK), pl.ds(pl.multiple_of(s * OWN, 128), OWN)],
                      o_send.at[k - 1, b], o_recv.at[k - 1, b], (dx, fz, t))

    def x_forward(lo, hi):
        def body(b):
            x_copy(0, b).wait_recv()
            x_copy(2, b).start()
        for_each(lo, hi, body)

    def norm(src, dst, row, lo, n):
        gains = jnp.concatenate([gbuf[j, row:row + 1, :] for j in range(NZ)], axis=-1).astype(jnp.float32)

        def body(i):
            h = src[at_rows(lo + i * BLK, BLK), :].astype(jnp.float32)
            inv = lax.rsqrt(jnp.mean(h * h, axis=-1, keepdims=True) + NORM_EPS)
            dst(i)[...] = (h * inv * gains).astype(jnp.bfloat16)

        for_each(0, n // BLK, body)

    def x_norm(part):
        if part == 0:
            for cp in g_copies():
                cp.wait_recv()
            g_own().wait()

        def body(b):
            x_copy(1, b).wait_recv()
            x_copy(2, b).wait_recv()
            x_copy(2, b).wait_send()
            x_own(b).wait()

        for_each(part * per, part * per + per, body)
        lo = part * per * SEQ
        norm(xa, lambda i: xa.at[at_rows(lo + i * BLK, BLK)], 0, lo, per * SEQ)

    def late_sends():
        def body(b):
            for k in range(2):
                x_copy(k, b).wait_send()
        for_each(0, ROWS, body)
        for cp in g_copies():
            cp.wait_send()
        res_load().wait()

    def piece(w, base, lo, width, slot, first, col):
        sh, g = shards[w], gathered[w]
        ks = sh.shape[0]
        cols = pl.ds(pl.multiple_of(lo, 128), width)
        out = []
        for j in range(NZ):
            src = sh.at[:, cols] if j == 0 else g.at[j, :, cols]
            at = pl.ds(pl.multiple_of(base + lax.rem(fz + j, NZ) * ks, 32), ks)
            out.append(pltpu.make_async_copy(src, wbuf.at[slot, at, col:col + width], wsem.at[slot, first + j]))
        return out

    def tiles(n, start, wait, compute):
        start(0, 0)

        def body(t):
            slot = lax.rem(t, 2)

            @pl.when(t + 1 < n)
            def _():
                start(t + 1, 1 - slot)

            wait(t, slot)
            compute(t, slot)

        for_each(0, n, body)

    def simple(n, load, compute):
        def start(t, slot):
            for cp in load(t, slot):
                cp.start()

        def wait(t, slot):
            for cp in load(t, slot):
                cp.wait()

        tiles(n, start, wait, compute)

    def by_rows(n, rows, body):
        for_each(0, n, lambda m: body(pl.ds(pl.multiple_of(m * rows, rows), rows)))

    m_rows = TOK // 2
    n_m = TOK // m_rows

    def qkv(part):
        rows = 2 * SEQ
        top = 3 * HEADS - 1

        def start(t, slot):
            for side in range(2):
                hh = jnp.minimum(2 * t + side, top)
                for j, w in enumerate((W_Q, W_K, W_V)):
                    @pl.when(lax.div(hh, HEADS) == j)
                    def _():
                        for cp in piece(w, 0, s * OWN + lax.rem(hh, HEADS) * 128, 128, slot, NZ * side, 128 * side):
                            cp.start()

        def wait(t, slot):
            for side in range(2):
                for cp in piece(W_Q, 0, s * OWN, 128, slot, NZ * side, 128 * side):
                    cp.wait()

        def compute(t, slot):
            def body(m):
                at = at_rows(part * per * SEQ + m * rows, rows)
                acc = jnp.dot(xa[at, :], wbuf[slot, 0:DIM, :], preferred_element_type=jnp.float32)
                cos, sin = cos_tab[...], sin_tab[...]
                for side in range(2):
                    p = acc[:, side * 128:(side + 1) * 128]
                    swapped = jnp.concatenate([p[:, 64:], p[:, :64]], axis=-1)
                    turned = 2 * t + side < 2 * HEADS
                    val = jnp.where(turned, p * cos + swapped * sin, p)
                    big[at, pl.ds(pl.multiple_of((2 * t + side) * 128, 128), 128)] = val.astype(jnp.bfloat16)

            for_each(0, per * SEQ // rows, body)

        tiles(8, start, wait, compute)

    def attention(part):
        def body(b):
            at = at_rows(b * SEQ, SEQ)
            for h in range(HEADS):
                q, k, v = (big[at, (j * HEADS + h) * 128:(j * HEADS + h + 1) * 128] for j in range(3))
                sc = lax.dot_general(q, k, (((1,), (1,)), ((), ())), preferred_element_type=jnp.float32)
                sc = jnp.where(keep[...] > 0, sc * HEAD_DIM ** -0.5, MASK_VALUE)
                e = jnp.exp(sc - jnp.max(sc, axis=-1, keepdims=True))
                tot = jnp.sum(e, axis=-1, keepdims=True)
                o = jnp.dot(e.astype(jnp.bfloat16), v, preferred_element_type=jnp.float32) / tot
                big[at, h * 128:(h + 1) * 128] = o.astype(jnp.bfloat16)

        for_each(part * per, part * per + per, body)

    def send_mix(part):
        def body(b):
            for k in range(1, SP):
                o_copy(k, b).start()
            mix[at_rows(b * BLK, BLK), pl.ds(pl.multiple_of(s * OWN, 128), OWN)] = big[at_rows(b * SEQ + s * BLK, BLK), 0:OWN]

        for_each(part * per, part * per + per, body)

    act_at = 3 * TOK

    def out_proj():
        def arrive(b):
            for k in range(1, SP):
                o_copy(k, b).wait_recv()
        for_each(0, ROWS, arrive)

        def load(t, slot):
            return piece(W_O, 0, t * TILE, TILE, slot, 0, 0)

        def compute(t, slot):
            cols = pl.ds(pl.multiple_of(t * TILE, 128), TILE)

            def body(at):
                acc = jnp.dot(mix[at, :], wbuf[slot, 0:DIM, :], preferred_element_type=jnp.float32)
                res[at, cols] = (res[at, cols].astype(jnp.float32) + acc).astype(jnp.bfloat16)

            by_rows(n_m, m_rows, body)

        simple(DIM // TILE, load, compute)
        norm(res, lambda i: xa.at[at_rows(act_at + i * BLK, BLK)], 1, 0, TOK)

        def gone(b):
            for k in range(1, SP):
                o_copy(k, b).wait_send()
        for_each(0, ROWS, gone)

    def gate_up(lo, width):
        def load(t, slot):
            return (piece(W_G, 0, lo + t * TILE, TILE, slot, 0, 0)
                    + piece(W_U, DIM, lo + t * TILE, TILE, slot, NZ, 0))

        def compute(t, slot):
            tile = lo // TILE + t
            blk = lax.div(tile, DIM // TILE)
            cols = pl.ds(pl.multiple_of(lax.rem(tile, DIM // TILE) * TILE, 128), TILE)

            def body(m):
                a = xa[pl.ds(pl.multiple_of(act_at + m * m_rows, m_rows), m_rows), :]
                g = jnp.dot(a, wbuf[slot, 0:DIM, :], preferred_element_type=jnp.float32)
                u = jnp.dot(a, wbuf[slot, DIM:2 * DIM, :], preferred_element_type=jnp.float32)
                at = pl.ds(pl.multiple_of(blk * TOK + m * m_rows, m_rows), m_rows)
                xa[at, cols] = (g / (1.0 + jnp.exp(-g)) * u).astype(jnp.bfloat16)

            for_each(0, n_m, body)

        simple(width // TILE, load, compute)

    def y_copy(t):
        cols = pl.ds(pl.multiple_of(t * TILE, 128), TILE)
        return pltpu.make_async_copy(mix.at[:, cols], y_out.at[:, cols], ysem.at[t])

    def down(lo, width):
        def load(t, slot):
            return piece(W_D, 0, lo + t * TILE, TILE, slot, 0, 0)

        def compute(t, slot):
            cols = pl.ds(pl.multiple_of(lo + t * TILE, 128), TILE)

            def body(m):
                acc = None
                for j in range(3):
                    n = min(DIM, FFN - j * DIM)
                    h = xa[pl.ds(pl.multiple_of(j * TOK + m * m_rows, m_rows), m_rows), 0:n]
                    d = jnp.dot(h, wbuf[slot, j * DIM:j * DIM + n, :], preferred_element_type=jnp.float32)
                    acc = d if acc is None else acc + d
                at = pl.ds(pl.multiple_of(m * m_rows, m_rows), m_rows)
                mix[at, cols] = (res[at, cols].astype(jnp.float32) + acc).astype(jnp.bfloat16)

            for_each(0, n_m, body)
            y_copy(lo // TILE + t).start()

        simple(width // TILE, load, compute)

    def begin(b):
        x_copy(0, b).start()
        x_copy(1, b).start()
        x_own(b).start()

    for cp in g_copies() + [g_own()]:
        cp.start()
    for_each(0, ROWS, begin)
    res_load().start()
    hooks = {}

    def hook(tick, fn, *args):
        hooks.setdefault(tick, []).append(functools.partial(fn, *args))

    last = {}
    for r, (w, lo, width) in enumerate(rounds):
        last[(w, lo)] = r + (2 if w <= W_V else LAG)
    for j, tick in enumerate(FORWARD_TICKS):
        hook(tick, x_forward, 3 * j, 3 * j + 3)
    tick = last[(W_V, 256)]
    for part in range(PARTS):
        hook(tick - 2 + part, x_norm, part)
    hook(tick, late_sends)
    for part in range(PARTS):
        hook(tick + part, qkv, part)
        hook(tick + part, attention, part)
        hook(tick + part, send_mix, part)
    tick = max(last[(W_O, HALF)], tick + PARTS + OUT_WAIT)
    hook(tick, out_proj)
    for w, lo, width in rounds:
        if w == W_U:
            tick = max(tick + 1, last[(w, lo)])
            hook(tick, gate_up, lo, width)
        if w == W_D:
            hook(last[(w, lo)], down, lo, width)
    for i in range(mv.ticks()):
        mv.step(i)
        for fn in hooks.get(i, ()):
            fn()
    for t in range(DIM // TILE):
        y_copy(t).wait()
    mv.finish()


def local_layer(x_loc, norm_attn, w_query, w_key, w_value, w_out, norm_mlp, w_gate, w_up, w_down):
    shards = (w_query, w_key, w_value, w_out, w_gate, w_up, w_down)
    gain = jnp.concatenate([norm_attn[None], norm_mlp[None], jnp.zeros((14, DIM // NZ), jnp.bfloat16)], axis=0)
    seq_idx = jnp.arange(SEQ, dtype=jnp.int32)
    pos = (seq_idx % BLK) * SP + seq_idx // BLK
    inv_freq = jnp.exp(jnp.arange(HEAD_DIM // 2, dtype=jnp.float32) * (-2.0 * math.log(ROPE_THETA) / HEAD_DIM))
    angles = pos.astype(jnp.float32)[:, None] * inv_freq[None, :]
    cos, sin = jnp.cos(angles), jnp.sin(angles)
    cos_tab = jnp.tile(jnp.concatenate([cos, cos], axis=-1), (2, 1))
    sin_tab = jnp.tile(jnp.concatenate([-sin, sin], axis=-1), (2, 1))
    keep = (pos[None, :] <= pos[:, None]).astype(jnp.float32)
    rounds, early = plan()
    any_spec = pl.BlockSpec(memory_space=pl.ANY)
    vmem_spec = pl.BlockSpec(memory_space=pltpu.VMEM)
    dma = pltpu.SemaphoreType.DMA
    bf16 = jnp.bfloat16
    outs = [jax.ShapeDtypeStruct((TOK, DIM), bf16)]
    outs += [jax.ShapeDtypeStruct((NZ,) + w.shape, bf16) for w in shards]
    res = pl.pallas_call(
        functools.partial(layer_kernel, rounds, early),
        out_shape=outs,
        in_specs=[any_spec, any_spec] + [vmem_spec] * 3 + [any_spec] * 7,
        out_specs=[any_spec] * 8,
        scratch_shapes=[
            pltpu.VMEM((ALL, DIM), bf16), pltpu.VMEM((ALL, 16 * 128), bf16), pltpu.VMEM((TOK, DIM), bf16),
            pltpu.VMEM((TOK, DIM), bf16), pltpu.VMEM((NZ, 16, DIM // NZ), bf16), pltpu.VMEM((2, FFN, TILE), bf16),
            dma((SLOTS, N_KINDS)), dma((SLOTS, N_KINDS)), dma((3, ROWS)), dma((3, ROWS)),
            dma((SP - 1, ROWS)), dma((SP - 1, ROWS)), dma((NZ - 1,)), dma((NZ - 1,)),
            dma((ROWS + 2,)), dma((2, 2 * NZ)), dma((DIM // TILE,))],
        compiler_params=pltpu.CompilerParams(has_side_effects=True, vmem_limit_bytes=60 * 1024 * 1024),
    )(x_loc.reshape(TOK, DIM), gain, cos_tab, sin_tab, keep, *shards)
    return res[0].reshape(x_loc.shape)


def solution(mesh):
    row_spec = P(('dp', 'fsdp'), 'sp', None)
    weight_spec = P('fsdp', None)
    gain_spec = P('fsdp')
    in_specs = (row_spec, gain_spec, weight_spec, weight_spec, weight_spec, weight_spec, gain_spec, weight_spec, weight_spec, weight_spec)
    return jax.shard_map(local_layer, mesh=mesh, in_specs=in_specs, out_specs=row_spec, check_vma=False)
```
